256 devices in a mesh: leaf: 256 (over x, y, z, core).
Axes of the slice: x: 4, y: 4, z: 8, core: 2. Of those that a mesh axis runs over, the one named last changes fastest.
Arguments:
- coarse_basis: float32 [9, 131072, 256], P(None, 'leaf'), as said below
- rhs_vectors_coarse: float32 [131072, 768], P('leaf'), may hold values from -6 to 6
- vertex_tier_depth: int32 [131072], P('leaf'), may hold values from 0 to 8
Outputs:
- solution: float32 [131072, 768], P('leaf')
The draws below stay inside these ranges and needn't reach their ends.
Inputs may be any that keep to these rules, and one draw needn't show every extreme that they name: vertex_tier_depth[v] is the coarsest separator level whose block has vertex v in its support; level 0 is the vertex's own leaf block. `coarse_basis`: float32 entries, finite.
All inputs are finite; a program needn't handle non-finite values.
Results may differ from the reference program's by a relative error of at most 0.0001.
Values sent between devices are 32-bit elements; how exact they have to be, the bound alone decides.
No kernel may reach another device: no remote copies, remote signals or barrier semaphores. Data moves between devices by JAX's collectives and lax.ppermute only.
A program may use at most 128 MiB of HBM per device.

```python
import jax
import jax.numpy as jnp
from jax import lax

S = 256
V_DEV = 512
NRHS = 768
LEVELS = 8
VERTS = 131072
N_LEAF = 256


def draw_coarse_basis(key, part):
    level_number = jnp.arange(LEVELS + 1).astype(jnp.float32)
    tier_scale_factor = (S * V_DEV * jnp.exp2(level_number)) ** (-0.25)
    entries = jax.random.normal(key, (LEVELS + 1, VERTS, S), jnp.float32)
    return (entries * tier_scale_factor[:, None, None]).astype(jnp.float32)


def set_ends(array, stream_key, least, largest):
    extent = array.shape
    place = [jax.random.randint(jax.random.fold_in(stream_key, axis), (), 0, extent[axis]) for axis in range(len(extent))]
    array = array.at[tuple(place)].set(least)
    longest = extent.index(max(extent))
    place[longest] = (place[longest] + 1) % extent[longest]
    return array.at[tuple(place)].set(largest)


def level_of(stream_key, dims, cuts, low, top_value):
    loudness = 1.0
    for dim, parts in cuts:
        heights = jax.random.uniform(jax.random.fold_in(jax.random.fold_in(stream_key, 6), dim), (parts,), jnp.float32, low / len(cuts), top_value / len(cuts))
        loudness = loudness * jnp.repeat(jnp.exp(heights), dims[dim] // parts).reshape((-1,) + (1,) * (len(dims) - 1 - dim))
    return loudness


def centred(rng, extent, scale, most, pieces=(), kind=jnp.bfloat16):
    gain = level_of(rng, extent, pieces, -0.22, 0.18) if pieces else 1.0
    drawn = jax.random.normal(rng, extent, jnp.float32) * scale * gain
    return jnp.minimum(jnp.maximum(drawn, -most), most).astype(kind)


def setup_inputs(seed: int = 0) -> dict:
    key_list = jax.random.split(jax.random.key(seed), 4)
    coarse_basis = draw_coarse_basis(jax.random.fold_in(key_list[3], 71), 0)
    rhs_vectors_coarse = centred(key_list[1], (VERTS, NRHS), 1.0, 6.0, ((0, 256),), jnp.float32)
    vertex_tier_depth = set_ends(jax.random.randint(key_list[2], (VERTS,), 0, LEVELS + 1), jax.random.fold_in(key_list[2], 1), 0, LEVELS).astype(jnp.int32)
    return {"coarse_basis": coarse_basis, "rhs_vectors_coarse": rhs_vectors_coarse, "vertex_tier_depth": vertex_tier_depth}


def reference(coarse_basis, rhs_vectors_coarse, vertex_tier_depth):
    vertex_count = coarse_basis.shape[1]
    solution = jnp.zeros((vertex_count, NRHS), jnp.float32)
    for level_number in range(LEVELS + 1):
        level_mask = (vertex_tier_depth >= level_number).astype(jnp.float32)
        level_basis = coarse_basis[level_number] * level_mask[:, None]
        group_count = N_LEAF // (2 ** level_number)
        grouped_basis = level_basis.reshape(group_count, -1, S)
        grouped_sides = rhs_vectors_coarse.reshape(group_count, -1, NRHS)
        coefficients = jnp.einsum("gvs,gvr->gsr", grouped_basis, grouped_sides, precision=lax.Precision.HIGHEST)
        image = jnp.einsum("gvs,gsr->gvr", grouped_basis, coefficients, precision=lax.Precision.HIGHEST)
        solution = solution + image.reshape(vertex_count, NRHS)
    return solution
```

```python
import functools

import jax
import jax.numpy as jnp
from jax import lax
from jax.experimental import pallas as pl
from jax.experimental.pallas import tpu as pltpu
from jax.sharding import PartitionSpec as P

N = 256
V = 512
S = 256
R = 768
UNIT = 48
UNITS = 16
OWN = ((6, 5, 4, 3), (8, 7, 2, 1))


def place(i):
    return i >> 6, (i >> 4) & 3, (i >> 1) & 7, i & 1


def index(x, y, z, core):
    return x << 6 | y << 4 | z << 1 | core


def pairs(*partners):
    out = []
    for i in range(N):
        x, y, z, core = place(i)
        if partners[core] is not None:
            out.append((i, index(*partners[core](x, y, z), core)))
    return out


def along_x(j):
    return lambda x, y, z: (x ^ j, y, z)


def along_y(j):
    return lambda x, y, z: (x, y ^ j, z)


def along_z(j):
    return lambda x, y, z: (x, y, z ^ j)


def shifted_z(j):
    return lambda x, y, z: (x, y, ((((z + 7) & 7) ^ j) + 1) & 7)


def send(array, perm):
    return lax.ppermute(array, "leaf", perm)


SWAP = [(i, i ^ 1) for i in range(N)]


def split(value):
    high = value.astype(jnp.bfloat16)
    low = (value - high.astype(jnp.float32)).astype(jnp.bfloat16)
    return high, low


def masked(basis, depth, level):
    keep = depth[...] >= level
    return jnp.concatenate(
        [jnp.where(keep, basis[:, :128], 0.0), jnp.where(keep, basis[:, 128:], 0.0)], 1
    )


def dot3(a_high, a_low, b_high, b_low, dims):
    dot = functools.partial(
        lax.dot_general, dimension_numbers=(dims, ((), ())), preferred_element_type=jnp.float32
    )
    return dot(a_high, b_high) + (dot(a_high, b_low) + dot(a_low, b_high))


def prepare_kernel(rhs, depth, high, low, depth_out):
    turned = rhs[...].T
    high[...], low[...] = split(turned)
    depth_out[...] = jnp.broadcast_to(depth[...].astype(jnp.float32), (128, V)).T


def prepare(rhs, depth):
    return pl.pallas_call(
        prepare_kernel,
        out_shape=(
            jax.ShapeDtypeStruct((R, V), jnp.bfloat16),
            jax.ShapeDtypeStruct((R, V), jnp.bfloat16),
            jax.ShapeDtypeStruct((V, 128), jnp.float32),
        ),
        name="prepare",
    )(rhs, depth.reshape(1, V))


def partial_kernel(levels, rows, basis, rhs_high, rhs_low, depth, out):
    slot = pl.program_id(0)
    high, low = split(masked(basis[0], depth, levels[slot].astype(jnp.float32)))
    product = dot3(rhs_high[...], rhs_low[...], high, low, ((1,), (0,)))
    for unit in range(UNITS):
        row = pl.multiple_of(rows[slot * UNITS + unit], 16)
        out[pl.ds(row, UNIT), :] = product[unit * UNIT : (unit + 1) * UNIT]


def partials(levels, rows, basis, rhs_high, rhs_low, depth, name):
    slots = levels.shape[0]
    whole = lambda shape: pl.BlockSpec(shape, lambda i, *_: (0,) * len(shape))
    return pl.pallas_call(
        partial_kernel,
        out_shape=jax.ShapeDtypeStruct((slots * R, S), jnp.float32),
        grid_spec=pltpu.PrefetchScalarGridSpec(
            num_scalar_prefetch=2,
            grid=(slots,),
            in_specs=[
                pl.BlockSpec((1, V, S), lambda i, levels, rows: (levels[i], 0, 0)),
                whole((R, V)),
                whole((R, V)),
                whole((V, 128)),
            ],
            out_specs=whole((slots * R, S)),
        ),
        cost_estimate=pl.CostEstimate(
            flops=slots * 6 * R * S * V, bytes_accessed=slots * 4 * S * (R + V), transcendentals=0
        ),
        name=name,
    )(levels, rows, basis, rhs_high, rhs_low, depth)


def leaf_kernel(basis, rhs_high, rhs_low, depth, out):
    high, low = split(masked(basis[0], depth, 0.0))
    product = dot3(rhs_high[...], rhs_low[...], high, low, ((1,), (0,)))
    out[...] = dot3(high, low, *split(product), ((1,), (1,)))


def leaf(basis, rhs_high, rhs_low, depth):
    whole = lambda shape: pl.BlockSpec(shape, lambda i: (0,) * len(shape))
    return pl.pallas_call(
        leaf_kernel,
        out_shape=jax.ShapeDtypeStruct((V, R), jnp.float32),
        grid=(1,),
        in_specs=[whole((1, V, S)), whole((R, V)), whole((R, V)), whole((V, 128))],
        out_specs=whole((V, R)),
        cost_estimate=pl.CostEstimate(flops=12 * R * S * V, bytes_accessed=4 * V * R, transcendentals=0),
        name="leaf",
    )(basis, rhs_high, rhs_low, depth)


def image_kernel(plan, levels, rows, basis, depth, before, *refs):
    pieces, out, high, low = refs[:-3], refs[-3], refs[-2], refs[-1]
    slot = pl.program_id(0)

    @pl.when(slot == 0)
    def _():
        out[...] = before[...]

    for number, parts in enumerate(plan):

        @pl.when(slot == number)
        def _(number=number, parts=parts):
            for unit, (piece, start) in enumerate(parts):
                row = pl.multiple_of(rows[number * UNITS + unit], 16)
                part_high, part_low = split(pieces[piece][start : start + UNIT, :])
                high[pl.ds(row, UNIT), :] = part_high
                low[pl.ds(row, UNIT), :] = part_low

    x_high, x_low = split(masked(basis[0], depth, levels[slot].astype(jnp.float32)))
    out[...] += dot3(x_high, x_low, high[...], low[...], ((1,), (1,)))


def images(plan, levels, rows, basis, depth, before, pieces, name):
    slots = len(plan)
    whole = lambda shape: pl.BlockSpec(shape, lambda i, *_: (0,) * len(shape))
    return pl.pallas_call(
        functools.partial(image_kernel, plan),
        out_shape=jax.ShapeDtypeStruct((V, R), jnp.float32),
        grid_spec=pltpu.PrefetchScalarGridSpec(
            num_scalar_prefetch=2,
            grid=(slots,),
            in_specs=[
                pl.BlockSpec((1, V, S), lambda i, levels, rows: (levels[i], 0, 0)),
                whole((V, 128)),
                whole((V, R)),
                *[whole(piece.shape) for piece in pieces],
            ],
            out_specs=whole((V, R)),
            scratch_shapes=[pltpu.VMEM((R, S), jnp.bfloat16), pltpu.VMEM((R, S), jnp.bfloat16)],
        ),
        cost_estimate=pl.CostEstimate(
            flops=slots * 6 * R * S * V, bytes_accessed=slots * 4 * S * (R + V), transcendentals=0
        ),
        name=name,
    )(levels, rows, basis, depth, before, *pieces)


ROW_A = [(0, 576)[u >> 2] + (u & 3) * 144 if u < 8 else 1152 + (u - 8) * UNIT for u in range(UNITS)]
ROW_B = [(u >> 3) * 576 + (u >> 1 & 3) * 144 + UNIT + (u & 1) * UNIT for u in range(UNITS)]
ROW_C = [u * UNIT for u in range(UNITS)]
ROW_D = [R + u * UNIT for u in range(UNITS)]


def body(coarse_basis, rhs_vectors_coarse, vertex_tier_depth):
    me = lax.axis_index("leaf")
    x, y, z, core = place(me)
    first = core == 0
    turned = (z + 7) & 7
    quarter = (turned & 1) << 1 | (turned >> 1 & 1)
    zero = jnp.zeros_like(me)
    masks = (
        (y << 2 | quarter, (y & 1) << 3 | quarter << 1, quarter << 2, (z & 1) << 3),
        (x << 2 | y, (x & 1) << 3 | y << 1, zero, zero),
    )
    mine = [jnp.where(first, a, b) for a, b in zip(*masks)]
    theirs = [jnp.where(first, b, a) for a, b in zip(*masks)]
    my_levels = jnp.where(first, jnp.array(OWN[0], jnp.int32), jnp.array(OWN[1], jnp.int32))
    their_levels = jnp.where(first, jnp.array(OWN[1], jnp.int32), jnp.array(OWN[0], jnp.int32))
    units = jnp.arange(UNITS, dtype=jnp.int32)

    def rows_of(table, mask):
        return jnp.sum(
            jnp.where((units[:, None] ^ mask) == units[None, :], jnp.array(table, jnp.int32)[None, :], 0), 1
        )

    def rows_pair(tables, pair):
        return jnp.concatenate([rows_of(t, m) for t, m in zip(tables, pair)])

    high, low, depth = prepare(rhs_vectors_coarse, vertex_tier_depth)
    part = lambda levels, rows, name: partials(levels, rows, coarse_basis, high, low, depth, name)
    send_ab = part(their_levels[:2], rows_pair((ROW_A, ROW_B), theirs[:2]), "send_ab")
    got_ab = send(send_ab, SWAP)
    keep_ab = part(my_levels[:2], rows_pair((ROW_A, ROW_B), mine[:2]), "keep_ab")
    send_cd = part(their_levels[2:], rows_pair((ROW_C, ROW_D), theirs[2:]), "send_cd")
    got_cd = send(send_cd, SWAP)
    keep_cd = part(my_levels[2:], rows_pair((ROW_C, ROW_D), mine[2:]), "keep_cd")

    step = [None] + [pairs(along_y(j), along_x(j)) for j in (1, 2, 3)]
    ab = keep_ab + got_ab
    r1 = send(ab[576:1152], step[1])
    r2 = send(ab[1152:1344], step[2])
    r3 = send(ab[1344:1536], step[3])
    both = (ab[:576] + r1).reshape(4, 144, S)
    both = jnp.concatenate(
        [both[:, :UNIT] + (r2 + r3).reshape(4, UNIT, S), both[:, UNIT:]], 1
    )
    y_step = [None] + [pairs(None, along_y(j)) for j in (1, 2, 3)]
    one = both[0] + send(both[1], y_step[1]) + send(both[2], y_step[2]) + send(both[3], y_step[3])
    for j in (1, 2, 4):
        one = one + send(one, pairs(None, along_z(j)))
    ones = jnp.stack([one] + [send(one, y_step[j]) for j in (1, 2, 3)])
    near, mid, far = pairs(shifted_z(1), None), pairs(shifted_z(2), None), pairs(along_z(4), None)
    zeros = both[:2] + send(both[2:], near)
    last = zeros[0] + send(zeros[1], mid)
    last = last + send(last, far)
    zeros = jnp.stack([last, send(last, mid)])
    zeros = jnp.concatenate([zeros, send(zeros, near)])
    done = jnp.where(first, zeros, ones)
    top = done[:, :UNIT].reshape(192, S)
    done = done.reshape(576, S)
    q1, q2, q3 = send(done, step[1]), send(top, step[2]), send(top, step[3])
    ab_pieces = (done, q1, q2, q3)

    cd = keep_cd + got_cd
    c, d = cd[:R], cd[R:]
    half = R // 2
    m1 = send(jnp.where(first, d[half:], c[half:]), pairs(along_z(1), along_z(1)))
    d_low = d[:half] + m1
    m2 = send(jnp.where(first, d_low, c[:half]), pairs(along_z(2), along_z(1)))
    d_low = d_low + m2
    m3 = send(d_low, pairs(along_z(1), None))
    c_one = jnp.concatenate([c[:half] + m2, c[half:] + m1])
    c_low = c[:half] + send(c[half:], near)
    c_low = c_low[:192] + send(c_low[192:], mid)
    c_low = c_low + send(c_low, far)
    c_low = jnp.concatenate([c_low, send(c_low, mid)])
    c_zero = jnp.concatenate([c_low, send(c_low, near)])
    c_done = jnp.where(first, c_zero, c_one)
    d_done = jnp.where(first, jnp.concatenate([d_low, m3]), d)
    cd_pieces = (c_done, d_done)

    their_cd = tuple(send(piece, SWAP) for piece in cd_pieces)
    their_ab = tuple(send(piece, SWAP) for piece in ab_pieces)

    result = leaf(coarse_basis, high, low, depth)
    back = lambda mask: UNIT * (units ^ mask)
    plan_c = lambda p: [(p, u * UNIT) for u in range(UNITS)]

    def plan_ab(table, p):
        out = []
        for row in table:
            piece = 0 if row < 576 else 1 if row < 1152 else 2 if row < 1344 else 3
            out.append((p + piece, row - (0, 576, 1152, 1344)[piece]))
        return out

    result = images(
        [plan_c(0), plan_c(1), plan_c(2), plan_c(3)],
        jnp.concatenate([my_levels[2:], their_levels[2:]]),
        jnp.concatenate([back(m) for m in (*mine[2:], *theirs[2:])]),
        coarse_basis, depth, result, cd_pieces + their_cd, "image_cd",
    )
    result = images(
        [plan_ab(ROW_A, 0), plan_ab(ROW_B, 0), plan_ab(ROW_A, 4), plan_ab(ROW_B, 4)],
        jnp.concatenate([my_levels[:2], their_levels[:2]]),
        jnp.concatenate([back(m) for m in (*mine[:2], *theirs[:2])]),
        coarse_basis, depth, result, ab_pieces + their_ab, "image_ab",
    )
    return result


def solution(mesh):
    in_specs = (P(None, "leaf", None), P("leaf", None), P("leaf"))
    out_specs = P("leaf", None)
    return jax.shard_map(body, mesh=mesh, in_specs=in_specs, out_specs=out_specs, check_vma=False)
```

```python
import functools

import jax
import jax.numpy as jnp
from jax import lax
from jax.experimental import pallas as pl
from jax.experimental.pallas import tpu as pltpu
from jax.sharding import PartitionSpec as P

N = 256
V = 512
S = 256
R = 768
UNIT = 16
UNITS = 16
VMEM = pl.BlockSpec(memory_space=pltpu.VMEM)
SMEM = pl.BlockSpec(memory_space=pltpu.SMEM)
HBM = pl.BlockSpec(memory_space=pltpu.HBM)


def place(i):
    return i >> 6, (i >> 4) & 3, (i >> 1) & 7, i & 1


def index(x, y, z, core):
    return x << 6 | y << 4 | z << 1 | core


def pairs(*partners):
    out = []
    for i in range(N):
        x, y, z, core = place(i)
        if partners[core] is not None:
            out.append((i, index(*partners[core](x, y, z), core)))
    return out


def along_x(j):
    return lambda x, y, z: (x ^ j, y, z)


def along_y(j):
    return lambda x, y, z: (x, y ^ j, z)


def along_z(j):
    return lambda x, y, z: (x, y, z ^ j)


def shifted_z(j):
    return lambda x, y, z: (x, y, ((((z + 7) & 7) ^ j) + 1) & 7)


def send(array, perm):
    return lax.ppermute(array, "leaf", perm)


SWAP = [(i, i ^ 1) for i in range(N)]


def slots(me, core):
    x, y, z, _ = place(me)
    turned = (z + 7) & 7
    low, mid = turned & 1, turned >> 1 & 1
    quarter = low ^ 3 * mid
    first = core == 0
    levels = (6 + 2 * core, 5 + 2 * core, 3 + core, 2 - core)
    masks = (
        jnp.where(first, y << 2 | quarter, x << 2 | y),
        jnp.where(first, (y & 1) << 3 | quarter << 1, (x & 1) << 3 | y << 1),
        jnp.where(first, (z & 1) << 3, (low << 1 | mid) << 2),
        jnp.zeros_like(z),
    )
    return levels, masks


def row_a(unit):
    chunk, quarter = unit >> 2, unit & 3
    return jnp.where(chunk < 2, chunk * 192 + quarter * 48, 256 + chunk * 64 + quarter * UNIT)


def row_b(unit):
    return (unit >> 3) * 192 + (unit >> 1 & 3) * 48 + UNIT + (unit & 1) * UNIT


def row_c(unit):
    return unit * UNIT


def row_d(unit):
    return S + unit * UNIT


ROWS = (row_a, row_b, row_c, row_d)


def split(value):
    high = value.astype(jnp.bfloat16)
    low = (value - high.astype(jnp.float32)).astype(jnp.bfloat16)
    return high, low


def masked(basis, depth, level):
    keep = depth[...] >= jnp.asarray(level).astype(jnp.float32)
    return split(
        jnp.concatenate([jnp.where(keep, basis[:, :128], 0.0), jnp.where(keep, basis[:, 128:], 0.0)], 1)
    )


def dot3(a, b, contract):
    dot = functools.partial(
        lax.dot_general,
        dimension_numbers=(((contract,), (0,)), ((), ())),
        preferred_element_type=jnp.float32,
    )
    return dot(a[0], b[0]) + (dot(a[0], b[1]) + dot(a[1], b[0]))


def put(product, out, slot, mask):
    for unit in range(UNITS):
        row = pl.multiple_of(ROWS[slot](unit ^ mask), UNIT)
        out[pl.ds(row, UNIT), :] = product[unit * UNIT : (unit + 1) * UNIT]


def first_kernel(me, depth, rhs_hbm, basis_hbm, out, high, low, depth_out, rhs, basis, sems):
    levels, masks = slots(me[0], 1 - (me[0] & 1))
    copies = [pltpu.make_async_copy(rhs_hbm, rhs, sems.at[0])]
    for slot in (0, 1):
        copies.append(pltpu.make_async_copy(basis_hbm.at[levels[slot]], basis.at[slot], sems.at[slot + 1]))
    for copy in copies:
        copy.start()
    depth_out[...] = jnp.broadcast_to(depth[...].astype(jnp.float32), (128, V)).T
    copies[0].wait()
    high[...], low[...] = split(rhs[...])
    for slot in (0, 1):
        copies[slot + 1].wait()
        product = dot3(masked(basis.at[slot][...], depth_out, levels[slot]), (high[...], low[...]), 0)
        put(product, out, slot, masks[slot])


def first_partials(me, depth, rhs, basis):
    return pl.pallas_call(
        first_kernel,
        out_shape=(
            jax.ShapeDtypeStruct((2 * S, R), jnp.float32),
            jax.ShapeDtypeStruct((V, R), jnp.bfloat16),
            jax.ShapeDtypeStruct((V, R), jnp.bfloat16),
            jax.ShapeDtypeStruct((V, 128), jnp.float32),
        ),
        in_specs=[SMEM, VMEM, HBM, HBM],
        out_specs=(VMEM,) * 4,
        scratch_shapes=[
            pltpu.VMEM((V, R), jnp.float32),
            pltpu.VMEM((2, V, S), jnp.float32),
            pltpu.SemaphoreType.DMA((3,)),
        ],
        compiler_params=pltpu.CompilerParams(vmem_limit_bytes=52 << 20),
        cost_estimate=pl.CostEstimate(flops=12 * R * S * V, bytes_accessed=2 * 4 * S * (R + V), transcendentals=0),
        name="send_ab",
    )(me, depth, rhs, basis)


def partial_kernel(work, me, high, low, depth, basis_hbm, *refs):
    outs, (basis, sems) = refs[:-2], refs[-2:]
    sides = [slots(me[0], me[0] & 1), slots(me[0], 1 - (me[0] & 1))]
    copies = []
    for number, (_, slot, other) in enumerate(work):
        copy = pltpu.make_async_copy(basis_hbm.at[sides[other][0][slot]], basis.at[number], sems.at[number])
        copy.start()
        copies.append(copy)
    for number, (out, slot, other) in enumerate(work):
        copies[number].wait()
        levels, masks = sides[other]
        product = dot3(masked(basis.at[number][...], depth, levels[slot]), (high[...], low[...]), 0)
        put(product, outs[out], slot, masks[slot])


def partials(work, me, high, low, depth, basis, name):
    count = 1 + max(out for out, _, _ in work)
    return pl.pallas_call(
        functools.partial(partial_kernel, work),
        out_shape=tuple(jax.ShapeDtypeStruct((2 * S, R), jnp.float32) for _ in range(count)),
        in_specs=[SMEM, VMEM, VMEM, VMEM, HBM],
        out_specs=(VMEM,) * count,
        scratch_shapes=[pltpu.VMEM((len(work), V, S), jnp.float32), pltpu.SemaphoreType.DMA((len(work),))],
        compiler_params=pltpu.CompilerParams(vmem_limit_bytes=45 << 20),
        cost_estimate=pl.CostEstimate(
            flops=len(work) * 6 * R * S * V, bytes_accessed=len(work) * 4 * S * (R + V), transcendentals=0
        ),
        name=name,
    )(me, high, low, depth, basis)


def leaf_kernel(high, low, depth, basis, out):
    own = masked(basis[0], depth, 0)
    out[...] = dot3(own, split(dot3(own, (high[...], low[...]), 0)), 1)


def leaf(high, low, depth, basis):
    return pl.pallas_call(
        leaf_kernel,
        out_shape=jax.ShapeDtypeStruct((V, R), jnp.float32),
        in_specs=[VMEM, VMEM, VMEM, VMEM],
        out_specs=VMEM,
        compiler_params=pltpu.CompilerParams(vmem_limit_bytes=16 << 20),
        cost_estimate=pl.CostEstimate(flops=12 * R * S * V, bytes_accessed=4 * V * R, transcendentals=0),
        name="leaf",
    )(high, low, depth, basis)


def image_kernel(work, me, depth, before, basis, *refs):
    pieces, (out, high, low) = refs[:-3], refs[-3:]
    sides = [slots(me[0], me[0] & 1), slots(me[0], 1 - (me[0] & 1))]
    for number, (slot, other, plan) in enumerate(work):
        levels, masks = sides[other]
        for unit, (piece, start) in enumerate(plan):
            row = pl.multiple_of(UNIT * (unit ^ masks[slot]), UNIT)
            part_high, part_low = split(pieces[piece][start : start + UNIT, :])
            high[number, pl.ds(row, UNIT), :] = part_high
            low[number, pl.ds(row, UNIT), :] = part_low
        own = masked(basis[levels[slot]], depth, levels[slot])
        image = dot3(own, (high[number], low[number]), 1)
        out[...] = (before[...] if number == 0 else out[...]) + image


def images(work, me, depth, before, basis, pieces, name):
    count = len(work)
    return pl.pallas_call(
        functools.partial(image_kernel, work),
        out_shape=jax.ShapeDtypeStruct((V, R), jnp.float32),
        in_specs=[SMEM, VMEM, VMEM, VMEM] + [VMEM] * len(pieces),
        out_specs=VMEM,
        scratch_shapes=[pltpu.VMEM((count, S, R), jnp.bfloat16), pltpu.VMEM((count, S, R), jnp.bfloat16)],
        compiler_params=pltpu.CompilerParams(vmem_limit_bytes=16 << 20),
        cost_estimate=pl.CostEstimate(
            flops=count * 6 * R * S * V, bytes_accessed=count * 4 * S * (R + V), transcendentals=0
        ),
        name=name,
    )(me, depth, before, basis, *pieces)


def plan_ab(slot):
    out = []
    for unit in range(UNITS):
        if slot == 0:
            chunk, quarter = unit >> 2, unit & 3
            out.append((chunk, quarter * 48 if chunk < 2 else quarter * UNIT))
        else:
            out.append((unit >> 3, (unit >> 1 & 3) * 48 + UNIT + (unit & 1) * UNIT))
    return out


def shift_pieces(plan, by):
    return [(piece + by, row) for piece, row in plan]


PLAN_C = [(u >> 3, (u & 7) * UNIT) for u in range(UNITS)]
PLAN_D = [(2, u * UNIT) for u in range(UNITS)]


def body(basis, rhs, vertex_tier_depth):
    index_here = lax.axis_index("leaf")
    first = (index_here & 1) == 0
    me = index_here.reshape(1)

    send_ab, high, low, depth = first_partials(me, vertex_tier_depth.reshape(1, V), rhs, basis)
    got_ab = send(send_ab, SWAP)
    keep_ab, send_cd, keep_cd = partials(
        [(0, 0, 0), (0, 1, 0), (1, 2, 1), (1, 3, 1), (2, 2, 0), (2, 3, 0)], me, high, low, depth, basis, "rest"
    )
    got_cd = send(send_cd, SWAP)

    step = [None] + [pairs(along_y(j), along_x(j)) for j in (1, 2, 3)]
    ab = keep_ab + got_ab
    r1 = send(ab[192:384], step[1])
    r2 = send(ab[384:448], step[2])
    r3 = send(ab[448:512], step[3])

    near, mid = pairs(along_z(1), shifted_z(1)), pairs(along_z(2), shifted_z(2))
    cd = keep_cd + got_cd
    c, d = cd[:S], cd[S:]
    c = c[:128] + send(c[128:], near)
    d = d + send(d, pairs(along_z(1), None))

    both = (ab[:192] + r1).reshape(4, 48, R)
    both = jnp.concatenate([both[:, :UNIT] + (r2 + r3).reshape(4, UNIT, R), both[:, UNIT:]], 1)
    t1 = send(both[1], pairs(shifted_z(1), along_y(1)))
    t2 = send(both[2], pairs(shifted_z(1), along_y(2)))
    t3 = send(both[3], pairs(None, along_y(3)))
    total = both[0] + t1
    total, passed = jnp.where(first, total, total + t2 + t3), both[3] + t2
    total_t = total + send(jnp.where(first, passed, total), pairs(shifted_z(2), along_z(1)))
    total = total_t + send(total_t, pairs(along_z(4), along_z(2)))
    other = send(total, pairs(shifted_z(2), along_z(4)))
    total = jnp.where(first, total, total + other)
    g1 = send(total, pairs(shifted_z(1), along_y(1)))
    g2 = send(jnp.where(first, other, total), pairs(shifted_z(1), along_y(2)))
    g3 = send(total, pairs(None, along_y(3)))
    done = jnp.stack([total, g1, g2, jnp.where(first, other, g3)])
    top = done[:, :UNIT].reshape(64, R)
    done = done.reshape(192, R)
    ab_pieces = (done, send(done, step[1]), send(top, step[2]), send(top, step[3]))

    m2 = send(c[64:], mid)
    c_low = jnp.where(first, c[:64], c[:64] + m2)
    m3 = send(c_low, pairs(along_z(2), along_z(4)))
    c_low = c_low + m3
    m4 = send(c_low, pairs(None, shifted_z(2)))
    c_half = jnp.concatenate([c_low, jnp.where(first, c[64:] + m2, m4)])
    cd_pieces = (c_half, send(c_half, near), d)

    their_cd = tuple(send(piece, SWAP) for piece in cd_pieces)
    their_ab = tuple(send(piece, SWAP) for piece in ab_pieces)

    result = leaf(high, low, depth, basis)
    result = images(
        [(2, 0, PLAN_C), (3, 0, PLAN_D), (2, 1, shift_pieces(PLAN_C, 3)), (3, 1, shift_pieces(PLAN_D, 3))],
        me, depth, result, basis, cd_pieces + their_cd, "image_cd",
    )
    result = images([(0, 0, plan_ab(0)), (1, 0, plan_ab(1))], me, depth, result, basis, ab_pieces, "image_own")
    return images([(0, 1, plan_ab(0)), (1, 1, plan_ab(1))], me, depth, result, basis, their_ab, "image_last")


def solution(mesh):
    in_specs = (P(None, "leaf", None), P("leaf", None), P("leaf"))
    out_specs = P("leaf", None)
    return jax.shard_map(body, mesh=mesh, in_specs=in_specs, out_specs=out_specs, check_vma=False)
```

```python
import functools

import jax
import jax.numpy as jnp
from jax import lax
from jax.experimental import pallas as pl
from jax.experimental.pallas import tpu as pltpu
from jax.sharding import PartitionSpec as P


N = 256
V = 512
S = 256
R = 768
UNIT = 16
UNITS = 16
VMEM = pl.BlockSpec(memory_space=pltpu.VMEM)
SMEM = pl.BlockSpec(memory_space=pltpu.SMEM)
HBM = pl.BlockSpec(memory_space=pltpu.HBM)


def place(i):
    return i >> 6, (i >> 4) & 3, (i >> 1) & 7, i & 1


def index(x, y, z, core):
    return x << 6 | y << 4 | z << 1 | core


def pairs(*partners):
    out = []
    for i in range(N):
        x, y, z, core = place(i)
        if partners[core] is not None:
            out.append((i, index(*partners[core](x, y, z), core)))
    return out


def along_x(j):
    return lambda x, y, z: (x ^ j, y, z)


def along_y(j):
    return lambda x, y, z: (x, y ^ j, z)


def along_z(j):
    return lambda x, y, z: (x, y, z ^ j)


def shifted_z(j):
    return lambda x, y, z: (x, y, ((((z + 7) & 7) ^ j) + 1) & 7)


def send(array, perm):
    return lax.ppermute(array, "leaf", perm)


SWAP = [(i, i ^ 1) for i in range(N)]


def slots(me, core):
    x, y, z, _ = place(me)
    turned = (z + 7) & 7
    low, mid = turned & 1, turned >> 1 & 1
    quarter = low ^ 3 * mid
    first = core == 0
    levels = (6 + 2 * core, 5 + 2 * core, 3 + core, 2 - core)
    masks = (
        jnp.where(first, y << 2 | quarter, x << 2 | y),
        jnp.where(first, (y & 1) << 3 | quarter << 1, (x & 1) << 3 | y << 1),
        jnp.where(first, (z & 1) << 3, (low << 1 | mid) << 2),
        jnp.zeros_like(z),
    )
    return levels, masks


def row_a(unit):
    chunk, quarter = unit >> 2, unit & 3
    return jnp.where(chunk < 2, chunk * 192 + quarter * 48, 256 + chunk * 64 + quarter * UNIT)


def row_b(unit):
    return (unit >> 3) * 192 + (unit >> 1 & 3) * 48 + UNIT + (unit & 1) * UNIT


def row_c(unit):
    return unit * UNIT


def row_d(unit):
    return S + unit * UNIT


ROWS = (row_a, row_b, row_c, row_d)


def split(value):
    high = value.astype(jnp.bfloat16)
    low = (value - high.astype(jnp.float32)).astype(jnp.bfloat16)
    return high, low


def masked(basis, depth, level):
    keep = depth[...] >= jnp.asarray(level).astype(jnp.float32)
    return split(
        jnp.concatenate([jnp.where(keep, basis[:, :128], 0.0), jnp.where(keep, basis[:, 128:], 0.0)], 1)
    )


def dot3(a, b, contract):
    dot = functools.partial(
        lax.dot_general,
        dimension_numbers=(((contract,), (0,)), ((), ())),
        preferred_element_type=jnp.float32,
    )
    return dot(a[0], b[0]) + (dot(a[0], b[1]) + dot(a[1], b[0]))


def put(product, out, slot, mask):
    for unit in range(UNITS):
        row = pl.multiple_of(ROWS[slot](unit ^ mask), UNIT)
        out[pl.ds(row, UNIT), :] = product[unit * UNIT : (unit + 1) * UNIT]


def first_kernel(me, depth_hbm, rhs_hbm, basis_hbm, out, high, low, depth_out, depth, rhs, basis, sems):
    levels, masks = slots(me[0], 1 - (me[0] & 1))
    copies = [pltpu.make_async_copy(rhs_hbm, rhs, sems.at[0])]
    for slot in (0, 1):
        copies.append(pltpu.make_async_copy(basis_hbm.at[levels[slot]], basis.at[slot], sems.at[slot + 1]))
    depth_copy = pltpu.make_async_copy(depth_hbm, depth, sems.at[3])
    depth_copy.start()
    for copy in copies:
        copy.start()
    depth_copy.wait()
    depth_out[...] = jnp.broadcast_to(depth[...].astype(jnp.float32), (128, V)).T
    copies[0].wait()
    high[...], low[...] = split(rhs[...])
    for slot in (0, 1):
        copies[slot + 1].wait()
        product = dot3(masked(basis.at[slot][...], depth_out, levels[slot]), (high[...], low[...]), 0)
        put(product, out, slot, masks[slot])


def first_partials(me, depth, rhs, basis):
    return pl.pallas_call(
        first_kernel,
        out_shape=(
            jax.ShapeDtypeStruct((2 * S, R), jnp.float32),
            jax.ShapeDtypeStruct((V, R), jnp.bfloat16),
            jax.ShapeDtypeStruct((V, R), jnp.bfloat16),
            jax.ShapeDtypeStruct((V, 128), jnp.float32),
        ),
        in_specs=[SMEM, HBM, HBM, HBM],
        out_specs=(VMEM,) * 4,
        scratch_shapes=[
            pltpu.VMEM((1, V), jnp.int32),
            pltpu.VMEM((V, R), jnp.float32),
            pltpu.VMEM((2, V, S), jnp.float32),
            pltpu.SemaphoreType.DMA((4,)),
        ],
        compiler_params=pltpu.CompilerParams(vmem_limit_bytes=50 << 20),
        cost_estimate=pl.CostEstimate(flops=12 * R * S * V, bytes_accessed=2 * 4 * S * (R + V), transcendentals=0),
        name="send_ab",
    )(me, depth, rhs, basis)


def partial_kernel(work, me, high, low, depth, basis, out):
    for slot, other in work:
        levels, masks = slots(me[0], (me[0] & 1) ^ other)
        product = dot3(masked(basis[levels[slot]], depth, levels[slot]), (high[...], low[...]), 0)
        put(product, out, slot, masks[slot])


def partials(work, me, high, low, depth, basis):
    return pl.pallas_call(
        functools.partial(partial_kernel, work),
        out_shape=jax.ShapeDtypeStruct((2 * S, R), jnp.float32),
        in_specs=[SMEM, VMEM, VMEM, VMEM, VMEM],
        out_specs=VMEM,
        compiler_params=pltpu.CompilerParams(vmem_limit_bytes=12 << 20),
        cost_estimate=pl.CostEstimate(
            flops=12 * R * S * V, bytes_accessed=8 * S * (R + V), transcendentals=0
        ),
    )(me, high, low, depth, basis)


def leaf_kernel(high, low, depth, basis, out):
    own = masked(basis[0], depth, 0)
    out[...] = dot3(own, split(dot3(own, (high[...], low[...]), 0)), 1)


def leaf(high, low, depth, basis):
    return pl.pallas_call(
        leaf_kernel,
        out_shape=jax.ShapeDtypeStruct((V, R), jnp.float32),
        in_specs=[VMEM, VMEM, VMEM, VMEM],
        out_specs=VMEM,
        compiler_params=pltpu.CompilerParams(vmem_limit_bytes=12 << 20),
        cost_estimate=pl.CostEstimate(flops=12 * R * S * V, bytes_accessed=4 * V * R, transcendentals=0),
        name="leaf",
    )(high, low, depth, basis)


def image_kernel(work, me, depth, before, basis_hbm, *refs):
    pieces, (out, basis, high, low, sems) = refs[:-5], refs[-5:]
    sides = [slots(me[0], (me[0] & 1) ^ other) for _, other, _ in work]
    copies = []
    for number, (slot, _, _) in enumerate(work):
        copy = pltpu.make_async_copy(basis_hbm.at[sides[number][0][slot]], basis.at[number], sems.at[number])
        copy.start()
        copies.append(copy)
    for number, (slot, _, plan) in enumerate(work):
        mask = sides[number][1][slot]
        for unit, (piece, start) in enumerate(plan):
            row = pl.multiple_of(UNIT * (unit ^ mask), UNIT)
            part_high, part_low = split(pieces[piece][start : start + UNIT, :])
            high[number, pl.ds(row, UNIT), :] = part_high
            low[number, pl.ds(row, UNIT), :] = part_low
    for copy in copies:
        copy.wait()
    for number, (slot, _, _) in enumerate(work):
        own = masked(basis.at[number][...], depth, sides[number][0][slot])
        image = dot3(own, (high[number], low[number]), 1)
        out[...] = (before[...] if number == 0 else out[...]) + image


def images(work, me, depth, before, basis, pieces):
    count = len(work)
    return pl.pallas_call(
        functools.partial(image_kernel, work),
        out_shape=jax.ShapeDtypeStruct((V, R), jnp.float32),
        in_specs=[SMEM, VMEM, VMEM, HBM] + [VMEM] * len(pieces),
        out_specs=VMEM,
        scratch_shapes=[
            pltpu.VMEM((count, V, S), jnp.float32),
            pltpu.VMEM((count, S, R), jnp.bfloat16),
            pltpu.VMEM((count, S, R), jnp.bfloat16),
            pltpu.SemaphoreType.DMA((count,)),
        ],
        compiler_params=pltpu.CompilerParams(vmem_limit_bytes=50 << 20),
        cost_estimate=pl.CostEstimate(
            flops=count * 6 * R * S * V, bytes_accessed=count * 4 * S * (R + V), transcendentals=0
        ),
    )(me, depth, before, basis, *pieces)


def plan_ab(slot):
    out = []
    for unit in range(UNITS):
        if slot == 0:
            chunk, quarter = unit >> 2, unit & 3
            out.append((chunk, quarter * 48 if chunk < 2 else quarter * UNIT))
        else:
            out.append((unit >> 3, (unit >> 1 & 3) * 48 + UNIT + (unit & 1) * UNIT))
    return out


def shift_pieces(plan, by):
    return [(piece + by, row) for piece, row in plan]


PLAN_C = [(u >> 3, (u & 7) * UNIT) for u in range(UNITS)]
PLAN_D = [(2, u * UNIT) for u in range(UNITS)]


def local(kernel, rows, *arrays):
    return pl.pallas_call(
        kernel,
        out_shape=tuple(jax.ShapeDtypeStruct((height, R), jnp.float32) for height in rows),
        in_specs=[VMEM] * len(arrays),
        out_specs=(VMEM,) * len(rows),
        compiler_params=pltpu.CompilerParams(vmem_limit_bytes=8 << 20),
    )(*arrays)


def cut_kernel(kept, got, *outs):
    start = 0
    for out in outs:
        part = slice(start, start + out.shape[0])
        out[...] = kept[part, :] + got[part, :]
        start = part.stop


def join_kernel(base, r1, r2, r3, *outs):
    for quarter, out in enumerate(outs):
        at = quarter * 48
        top = slice(quarter * UNIT, (quarter + 1) * UNIT)
        out[:UNIT, :] = (base[at : at + UNIT, :] + r1[at : at + UNIT, :]) + (r2[top, :] + r3[top, :])
        out[UNIT:, :] = base[at + UNIT : at + 48, :] + r1[at + UNIT : at + 48, :]


def steps(basis, rhs, vertex_tier_depth):
    index_here = lax.axis_index("leaf")
    first = (index_here & 1) == 0
    me = index_here.reshape(1)

    send_ab, high, low, depth = first_partials(me, vertex_tier_depth.reshape(1, V), rhs, basis)
    got_ab = send(send_ab, SWAP)
    keep_ab = partials([(0, 0), (1, 0)], me, high, low, depth, basis)

    step = [None] + [pairs(along_y(j), along_x(j)) for j in (1, 2, 3)]
    base, s1, s2, s3 = local(cut_kernel, (192, 192, 64, 64), keep_ab, got_ab)
    r1 = send(s1, step[1])
    r2 = send(s2, step[2])
    r3 = send(s3, step[3])

    send_cd = partials([(2, 1), (3, 1)], me, high, low, depth, basis)
    got_cd = send(send_cd, SWAP)
    keep_cd = partials([(2, 0), (3, 0)], me, high, low, depth, basis)
    near, mid = pairs(along_z(1), shifted_z(1)), pairs(along_z(2), shifted_z(2))
    c_low, c_high, d = local(cut_kernel, (128, 128, 256), keep_cd, got_cd)
    c = c_low + send(c_high, near)
    d = d + send(d, pairs(along_z(1), None))

    both = local(join_kernel, (48,) * 4, base, r1, r2, r3)
    t1 = send(both[1], pairs(shifted_z(1), along_y(1)))
    t2 = send(both[2], pairs(shifted_z(1), along_y(2)))
    t3 = send(both[3], pairs(None, along_y(3)))
    total = both[0] + t1
    total, passed = jnp.where(first, total, total + t2 + t3), both[3] + t2
    total_t = total + send(jnp.where(first, passed, total), pairs(shifted_z(2), along_z(1)))
    total = total_t + send(total_t, pairs(along_z(4), along_z(2)))
    other = send(total, pairs(shifted_z(2), along_z(4)))
    total = jnp.where(first, total, total + other)
    g1 = send(total, pairs(shifted_z(1), along_y(1)))
    g2 = send(jnp.where(first, other, total), pairs(shifted_z(1), along_y(2)))
    g3 = send(total, pairs(None, along_y(3)))
    done = jnp.stack([total, g1, g2, jnp.where(first, other, g3)])
    top = done[:, :UNIT].reshape(64, R)
    done = done.reshape(192, R)
    q1, q2, q3 = send(done, step[1]), send(top, step[2]), send(top, step[3])
    ab_pieces = (done, q1, q2, q3)

    m2 = send(c[64:], mid)
    c_low = jnp.where(first, c[:64], c[:64] + m2)
    m3 = send(c_low, pairs(along_z(2), along_z(4)))
    c_low = c_low + m3
    m4 = send(c_low, pairs(None, shifted_z(2)))
    c_half = jnp.concatenate([c_low, jnp.where(first, c[64:] + m2, m4)])
    cd_pieces = (c_half, send(c_half, near), d)

    their_cd = tuple(send(piece, SWAP) for piece in cd_pieces)
    their_ab = tuple(send(piece, SWAP) for piece in ab_pieces)

    result = leaf(high, low, depth, basis)
    result = images(
        [(2, 0, PLAN_C), (3, 0, PLAN_D), (2, 1, shift_pieces(PLAN_C, 3)), (3, 1, shift_pieces(PLAN_D, 3))],
        me, depth, result, basis, cd_pieces + their_cd,
    )
    result = images([(0, 0, plan_ab(0)), (1, 0, plan_ab(1))], me, depth, result, basis, ab_pieces)
    return images([(0, 1, plan_ab(0)), (1, 1, plan_ab(1))], me, depth, result, basis, their_ab)


def solution(mesh):
    in_specs = (P(None, "leaf", None), P("leaf", None), P("leaf"))
    out_specs = P("leaf", None)
    return jax.shard_map(steps, mesh=mesh, in_specs=in_specs, out_specs=out_specs, check_vma=False)
```

```python
import functools

import jax
import jax.numpy as jnp
from jax import lax
from jax.experimental import pallas as pl
from jax.experimental.pallas import tpu as pltpu
from jax.sharding import PartitionSpec as P


N = 256
V = 512
S = 256
R = 768
UNIT = 16
UNITS = 16
VMEM = pl.BlockSpec(memory_space=pltpu.VMEM)
SMEM = pl.BlockSpec(memory_space=pltpu.SMEM)
HBM = pl.BlockSpec(memory_space=pltpu.HBM)


def place(i):
    return i >> 6, (i >> 4) & 3, (i >> 1) & 7, i & 1


def index(x, y, z, core):
    return x << 6 | y << 4 | z << 1 | core


def pairs(*partners):
    out = []
    for i in range(N):
        x, y, z, core = place(i)
        if partners[core] is not None:
            out.append((i, index(*partners[core](x, y, z), core)))
    return out


def along_x(j):
    return lambda x, y, z: (x ^ j, y, z)


def along_y(j):
    return lambda x, y, z: (x, y ^ j, z)


def along_z(j):
    return lambda x, y, z: (x, y, z ^ j)


def shifted_z(j):
    return lambda x, y, z: (x, y, ((((z + 7) & 7) ^ j) + 1) & 7)


def send(array, perm):
    return lax.ppermute(array, "leaf", perm)


SWAP = [(i, i ^ 1) for i in range(N)]


def slots(me, core):
    x, y, z, _ = place(me)
    turned = (z + 7) & 7
    low, mid = turned & 1, turned >> 1 & 1
    quarter = low ^ 3 * mid
    first = core == 0
    levels = (6 + 2 * core, 5 + 2 * core, 3 + core, 2 - core)
    masks = (
        jnp.where(first, y << 2 | quarter, x << 2 | y),
        jnp.where(first, (y & 1) << 3 | quarter << 1, (x & 1) << 3 | y << 1),
        jnp.where(first, (z & 1) << 3, (low << 1 | mid) << 2),
        jnp.zeros_like(z),
    )
    return levels, masks


def row_a(unit):
    chunk, quarter = unit >> 2, unit & 3
    return jnp.where(chunk < 2, chunk * 192 + quarter * 48, 256 + chunk * 64 + quarter * UNIT)


def row_b(unit):
    return (unit >> 3) * 192 + (unit >> 1 & 3) * 48 + UNIT + (unit & 1) * UNIT


def row_c(unit):
    return unit * UNIT


def row_d(unit):
    return S + unit * UNIT


ROWS = (row_a, row_b, row_c, row_d)


def split(value):
    high = value.astype(jnp.bfloat16)
    low = (value - high.astype(jnp.float32)).astype(jnp.bfloat16)
    return high, low


def masked(basis, depth, level):
    keep = depth[...] >= jnp.asarray(level).astype(jnp.float32)
    return split(
        jnp.concatenate([jnp.where(keep, basis[:, :128], 0.0), jnp.where(keep, basis[:, 128:], 0.0)], 1)
    )


def dot3(a, b, contract):
    dot = functools.partial(
        lax.dot_general,
        dimension_numbers=(((contract,), (0,)), ((), ())),
        preferred_element_type=jnp.float32,
    )
    return dot(a[0], b[0]) + (dot(a[0], b[1]) + dot(a[1], b[0]))


def put(product, out, slot, mask):
    for unit in range(UNITS):
        row = pl.multiple_of(ROWS[slot](unit ^ mask), UNIT)
        out[pl.ds(row, UNIT), :] = product[unit * UNIT : (unit + 1) * UNIT]


def first_kernel(me, depth_hbm, rhs_hbm, basis_hbm, out, high, low, depth_out, depth, rhs, basis, sems):
    levels, masks = slots(me[0], 1 - (me[0] & 1))
    copies = [pltpu.make_async_copy(rhs_hbm, rhs, sems.at[0])]
    for slot in (0, 1):
        copies.append(pltpu.make_async_copy(basis_hbm.at[levels[slot]], basis.at[slot], sems.at[slot + 1]))
    depth_copy = pltpu.make_async_copy(depth_hbm, depth, sems.at[3])
    depth_copy.start()
    for copy in copies:
        copy.start()
    depth_copy.wait()
    depth_out[...] = jnp.broadcast_to(depth[...].astype(jnp.float32), (128, V)).T
    copies[0].wait()
    high[...], low[...] = split(rhs[...])
    for slot in (0, 1):
        copies[slot + 1].wait()
        product = dot3(masked(basis.at[slot][...], depth_out, levels[slot]), (high[...], low[...]), 0)
        put(product, out, slot, masks[slot])


def first_partials(me, depth, rhs, basis):
    return pl.pallas_call(
        first_kernel,
        out_shape=(
            jax.ShapeDtypeStruct((2 * S, R), jnp.float32),
            jax.ShapeDtypeStruct((V, R), jnp.bfloat16),
            jax.ShapeDtypeStruct((V, R), jnp.bfloat16),
            jax.ShapeDtypeStruct((V, 128), jnp.float32),
        ),
        in_specs=[SMEM, HBM, HBM, HBM],
        out_specs=(VMEM,) * 4,
        scratch_shapes=[
            pltpu.VMEM((1, V), jnp.int32),
            pltpu.VMEM((V, R), jnp.float32),
            pltpu.VMEM((2, V, S), jnp.float32),
            pltpu.SemaphoreType.DMA((4,)),
        ],
        compiler_params=pltpu.CompilerParams(vmem_limit_bytes=50 << 20),
        cost_estimate=pl.CostEstimate(flops=12 * R * S * V, bytes_accessed=2 * 4 * S * (R + V), transcendentals=0),
        name="send_ab",
    )(me, depth, rhs, basis)


def partial_kernel(work, me, high, low, depth, basis, out):
    for slot, other in work:
        levels, masks = slots(me[0], (me[0] & 1) ^ other)
        product = dot3(masked(basis[levels[slot]], depth, levels[slot]), (high[...], low[...]), 0)
        put(product, out, slot, masks[slot])


def partials(work, me, high, low, depth, basis):
    return pl.pallas_call(
        functools.partial(partial_kernel, work),
        out_shape=jax.ShapeDtypeStruct((2 * S, R), jnp.float32),
        in_specs=[SMEM, VMEM, VMEM, VMEM, VMEM],
        out_specs=VMEM,
        compiler_params=pltpu.CompilerParams(vmem_limit_bytes=12 << 20),
        cost_estimate=pl.CostEstimate(
            flops=12 * R * S * V, bytes_accessed=8 * S * (R + V), transcendentals=0
        ),
    )(me, high, low, depth, basis)


def image_kernel(work, fresh, me, depth, basis, *refs):
    given, pieces, (out, high, low) = refs[: 2 if fresh else 1], refs[2 if fresh else 1 : -3], refs[-3:]
    if fresh:
        own = masked(basis[0], depth, 0)
        out[...] = dot3(own, split(dot3(own, (given[0][...], given[1][...]), 0)), 1)
    for number, (slot, other, plan) in enumerate(work):
        levels, masks = slots(me[0], (me[0] & 1) ^ other)
        for unit, (piece, start) in enumerate(plan):
            row = pl.multiple_of(UNIT * (unit ^ masks[slot]), UNIT)
            part_high, part_low = split(pieces[piece][start : start + UNIT, :])
            high[number, pl.ds(row, UNIT), :] = part_high
            low[number, pl.ds(row, UNIT), :] = part_low
        own = masked(basis[levels[slot]], depth, levels[slot])
        image = dot3(own, (high[number], low[number]), 1)
        out[...] = (out[...] if fresh or number else given[0][...]) + image


def images(work, fresh, limit, me, depth, basis, given, pieces):
    count = len(work)
    return pl.pallas_call(
        functools.partial(image_kernel, work, fresh),
        out_shape=jax.ShapeDtypeStruct((V, R), jnp.float32),
        in_specs=[SMEM] + [VMEM] * (2 + len(given) + len(pieces)),
        out_specs=VMEM,
        scratch_shapes=[pltpu.VMEM((count, S, R), jnp.bfloat16), pltpu.VMEM((count, S, R), jnp.bfloat16)],
        compiler_params=pltpu.CompilerParams(vmem_limit_bytes=limit << 20),
        cost_estimate=pl.CostEstimate(
            flops=(count + 2 * fresh) * 6 * R * S * V, bytes_accessed=count * 4 * S * (R + V), transcendentals=0
        ),
    )(me, depth, basis, *given, *pieces)


def plan_ab(slot):
    out = []
    for unit in range(UNITS):
        if slot == 0:
            chunk, quarter = unit >> 2, unit & 3
            out.append((chunk, quarter * 48 if chunk < 2 else quarter * UNIT))
        else:
            out.append((unit >> 3, (unit >> 1 & 3) * 48 + UNIT + (unit & 1) * UNIT))
    return out


def shift_pieces(plan, by):
    return [(piece + by, row) for piece, row in plan]


PLAN_C = [(u >> 3, (u & 7) * UNIT) for u in range(UNITS)]
PLAN_D = [(2, u * UNIT) for u in range(UNITS)]


def local(kernel, rows, *arrays):
    return pl.pallas_call(
        kernel,
        out_shape=tuple(jax.ShapeDtypeStruct((height, R), jnp.float32) for height in rows),
        in_specs=[SMEM if array.ndim == 1 else VMEM for array in arrays],
        out_specs=(VMEM,) * len(rows),
        compiler_params=pltpu.CompilerParams(vmem_limit_bytes=4 << 20),
    )(*arrays)


def cut_kernel(kept, got, *outs):
    start = 0
    for out in outs:
        part = slice(start, start + out.shape[0])
        out[...] = kept[part, :] + got[part, :]
        start = part.stop


def join_kernel(base, r1, r2, r3, *outs):
    for quarter, out in enumerate(outs):
        at = quarter * 48
        top = slice(quarter * UNIT, (quarter + 1) * UNIT)
        out[:UNIT, :] = (base[at : at + UNIT, :] + r1[at : at + UNIT, :]) + (r2[top, :] + r3[top, :])
        out[UNIT:, :] = base[at + UNIT : at + 48, :] + r1[at + UNIT : at + 48, :]


def by_core(me, zero, one):
    @pl.when((me[0] & 1) == 0)
    def _():
        zero()

    @pl.when((me[0] & 1) == 1)
    def _():
        one()


def settle_kernel(me, u0, u3, t1, t2, t3, total, passed):
    def zero():
        total[...] = u0[...] + t1[...]
        passed[...] = u3[...] + t2[...]

    def one():
        total[...] = (u0[...] + t1[...]) + (t2[...] + t3[...])
        passed[...] = total[...]

    by_core(me, zero, one)


def finish_kernel(me, total, other, out, passed):
    def zero():
        out[...] = total[...]
        passed[...] = other[...]

    def one():
        out[...] = total[...] + other[...]
        passed[...] = out[...]

    by_core(me, zero, one)


def stack_kernel(me, total, g1, g2, g3, other, done, top):
    for quarter, part in enumerate((total, g1, g2)):
        done[quarter * 48 : (quarter + 1) * 48, :] = part[...]
        top[quarter * UNIT : (quarter + 1) * UNIT, :] = part[:UNIT, :]

    def last(part):
        done[144:, :] = part[...]
        top[48:, :] = part[:UNIT, :]

    by_core(me, lambda: last(other), lambda: last(g3))


def half_kernel(me, c, m2, out):
    def zero():
        out[...] = c[...]

    def one():
        out[...] = c[...] + m2[...]

    by_core(me, zero, one)


def whole_kernel(me, c_low, c_high, m2, m4, out):
    out[:64, :] = c_low[...]

    def zero():
        out[64:, :] = c_high[...] + m2[...]

    def one():
        out[64:, :] = m4[...]

    by_core(me, zero, one)


def steps(basis, rhs, vertex_tier_depth):
    index_here = lax.axis_index("leaf")
    me = index_here.reshape(1)

    send_ab, high, low, depth = first_partials(me, vertex_tier_depth.reshape(1, V), rhs, basis)
    got_ab = send(send_ab, SWAP)
    keep_ab = partials([(0, 0), (1, 0)], me, high, low, depth, basis)

    step = [None] + [pairs(along_y(j), along_x(j)) for j in (1, 2, 3)]
    base, s1, s2, s3 = local(cut_kernel, (192, 192, 64, 64), keep_ab, got_ab)
    r1 = send(s1, step[1])
    r2 = send(s2, step[2])
    r3 = send(s3, step[3])

    send_cd = partials([(2, 1), (3, 1)], me, high, low, depth, basis)
    got_cd = send(send_cd, SWAP)
    keep_cd = partials([(2, 0), (3, 0)], me, high, low, depth, basis)
    near, mid = pairs(along_z(1), shifted_z(1)), pairs(along_z(2), shifted_z(2))
    c_low, c_high, d = local(cut_kernel, (128, 128, 256), keep_cd, got_cd)
    c_low, c_high = local(cut_kernel, (64, 64), c_low, send(c_high, near))
    d = d + send(d, pairs(along_z(1), None))

    u0, u1, u2, u3 = local(join_kernel, (48,) * 4, base, r1, r2, r3)
    t1 = send(u1, pairs(shifted_z(1), along_y(1)))
    t2 = send(u2, pairs(shifted_z(1), along_y(2)))
    t3 = send(u3, pairs(None, along_y(3)))
    total, passed = local(settle_kernel, (48, 48), me, u0, u3, t1, t2, t3)
    total = total + send(passed, pairs(shifted_z(2), along_z(1)))
    total = total + send(total, pairs(along_z(4), along_z(2)))
    other = send(total, pairs(shifted_z(2), along_z(4)))
    total, passed = local(finish_kernel, (48, 48), me, total, other)
    g1 = send(total, pairs(shifted_z(1), along_y(1)))
    g2 = send(passed, pairs(shifted_z(1), along_y(2)))
    g3 = send(total, pairs(None, along_y(3)))
    done, top = local(stack_kernel, (192, 64), me, total, g1, g2, g3, other)
    q1, q2, q3 = send(done, step[1]), send(top, step[2]), send(top, step[3])
    ab_pieces = (done, q1, q2, q3)

    m2 = send(c_high, mid)
    (c_low,) = local(half_kernel, (64,), me, c_low, m2)
    c_low = c_low + send(c_low, pairs(along_z(2), along_z(4)))
    m4 = send(c_low, pairs(None, shifted_z(2)))
    (c_half,) = local(whole_kernel, (128,), me, c_low, c_high, m2, m4)
    cd_pieces = (c_half, send(c_half, near), d)

    their_cd = tuple(send(piece, SWAP) for piece in cd_pieces)
    their_ab = tuple(send(piece, SWAP) for piece in ab_pieces)

    result = images(
        [(2, 0, PLAN_C), (3, 0, PLAN_D), (2, 1, shift_pieces(PLAN_C, 3)), (3, 1, shift_pieces(PLAN_D, 3))],
        True, 16, me, depth, basis, (high, low), cd_pieces + their_cd,
    )
    result = images([(0, 0, plan_ab(0)), (1, 0, plan_ab(1))], False, 12, me, depth, basis, (result,), ab_pieces)
    return images([(0, 1, plan_ab(0)), (1, 1, plan_ab(1))], False, 12, me, depth, basis, (result,), their_ab)


def solution(mesh):
    in_specs = (P(None, "leaf", None), P("leaf", None), P("leaf"))
    out_specs = P("leaf", None)
    return jax.shard_map(steps, mesh=mesh, in_specs=in_specs, out_specs=out_specs, check_vma=False)
```

```python
import functools

import jax
import jax.numpy as jnp
from jax import lax
from jax.experimental import pallas as pl
from jax.experimental.pallas import tpu as pltpu
from jax.sharding import PartitionSpec as P


N = 256
V = 512
S = 256
R = 768
UNIT = 16
UNITS = 16
VMEM = pl.BlockSpec(memory_space=pltpu.VMEM)
SMEM = pl.BlockSpec(memory_space=pltpu.SMEM)
HBM = pl.BlockSpec(memory_space=pltpu.HBM)


def place(i):
    return i >> 6, (i >> 4) & 3, (i >> 1) & 7, i & 1


def index(x, y, z, core):
    return x << 6 | y << 4 | z << 1 | core


def pairs(*partners):
    out = []
    for i in range(N):
        x, y, z, core = place(i)
        if partners[core] is not None:
            out.append((i, index(*partners[core](x, y, z), core)))
    return out


def along_x(j):
    return lambda x, y, z: (x ^ j, y, z)


def along_y(j):
    return lambda x, y, z: (x, y ^ j, z)


def along_z(j):
    return lambda x, y, z: (x, y, z ^ j)


def shifted_z(j):
    return lambda x, y, z: (x, y, ((((z + 7) & 7) ^ j) + 1) & 7)


def send(array, perm):
    return lax.ppermute(array, "leaf", perm)


SWAP = [(i, i ^ 1) for i in range(N)]


def slots(me, core):
    x, y, z, _ = place(me)
    turned = (z + 7) & 7
    low, mid = turned & 1, turned >> 1 & 1
    quarter = low ^ 3 * mid
    first = core == 0
    levels = (6 + 2 * core, 5 + 2 * core, 3 + core, 2 - core)
    masks = (
        jnp.where(first, y << 2 | quarter, x << 2 | y),
        jnp.where(first, (y & 1) << 3 | quarter << 1, (x & 1) << 3 | y << 1),
        jnp.where(first, (z & 1) << 3, (low << 1 | mid) << 2),
        jnp.zeros_like(z),
    )
    return levels, masks


def row_a(unit):
    chunk, quarter = unit >> 2, unit & 3
    return jnp.where(chunk < 2, chunk * 192 + quarter * 48, 256 + chunk * 64 + quarter * UNIT)


def row_b(unit):
    return (unit >> 3) * 192 + (unit >> 1 & 3) * 48 + UNIT + (unit & 1) * UNIT


def row_c(unit):
    return unit * UNIT


def row_d(unit):
    return S + unit * UNIT


ROWS = (row_a, row_b, row_c, row_d)


def split(value):
    high = value.astype(jnp.bfloat16)
    low = (value - high.astype(jnp.float32)).astype(jnp.bfloat16)
    return high, low


def masked(basis, depth, level):
    keep = depth[...] >= jnp.asarray(level).astype(jnp.float32)
    return split(
        jnp.concatenate([jnp.where(keep, basis[:, :128], 0.0), jnp.where(keep, basis[:, 128:], 0.0)], 1)
    )


def dot3(a, b, contract):
    dot = functools.partial(
        lax.dot_general,
        dimension_numbers=(((contract,), (0,)), ((), ())),
        preferred_element_type=jnp.float32,
    )
    return dot(a[0], b[0]) + (dot(a[0], b[1]) + dot(a[1], b[0]))


def put(product, out, slot, mask):
    for unit in range(UNITS):
        row = pl.multiple_of(ROWS[slot](unit ^ mask), UNIT)
        out[pl.ds(row, UNIT), :] = product[unit * UNIT : (unit + 1) * UNIT]


def first_kernel(me, depth_hbm, rhs_hbm, basis_hbm, out, high, low, depth_out, depth, rhs, basis, sems):
    levels, masks = slots(me[0], 1 - (me[0] & 1))
    copies = [pltpu.make_async_copy(rhs_hbm, rhs, sems.at[0])]
    for slot in (0, 1):
        copies.append(pltpu.make_async_copy(basis_hbm.at[levels[slot]], basis.at[slot], sems.at[slot + 1]))
    depth_copy = pltpu.make_async_copy(depth_hbm, depth, sems.at[3])
    depth_copy.start()
    for copy in copies:
        copy.start()
    depth_copy.wait()
    depth_out[...] = jnp.broadcast_to(depth[...].astype(jnp.float32), (128, V)).T
    copies[0].wait()
    high[...], low[...] = split(rhs[...])
    for slot in (0, 1):
        copies[slot + 1].wait()
        product = dot3(masked(basis.at[slot][...], depth_out, levels[slot]), (high[...], low[...]), 0)
        put(product, out, slot, masks[slot])


def first_partials(me, depth, rhs, basis):
    return pl.pallas_call(
        first_kernel,
        out_shape=(
            jax.ShapeDtypeStruct((2 * S, R), jnp.float32),
            jax.ShapeDtypeStruct((V, R), jnp.bfloat16),
            jax.ShapeDtypeStruct((V, R), jnp.bfloat16),
            jax.ShapeDtypeStruct((V, 128), jnp.float32),
        ),
        in_specs=[SMEM, HBM, HBM, HBM],
        out_specs=(VMEM,) * 4,
        scratch_shapes=[
            pltpu.VMEM((1, V), jnp.int32),
            pltpu.VMEM((V, R), jnp.float32),
            pltpu.VMEM((2, V, S), jnp.float32),
            pltpu.SemaphoreType.DMA((4,)),
        ],
        compiler_params=pltpu.CompilerParams(vmem_limit_bytes=50 << 20),
        cost_estimate=pl.CostEstimate(flops=12 * R * S * V, bytes_accessed=2 * 4 * S * (R + V), transcendentals=0),
        name="send_ab",
    )(me, depth, rhs, basis)


def partial_kernel(work, me, high, low, depth, basis, out):
    for slot, other in work:
        levels, masks = slots(me[0], (me[0] & 1) ^ other)
        product = dot3(masked(basis[levels[slot]], depth, levels[slot]), (high[...], low[...]), 0)
        put(product, out, slot, masks[slot])


def partials(work, me, high, low, depth, basis):
    return pl.pallas_call(
        functools.partial(partial_kernel, work),
        out_shape=jax.ShapeDtypeStruct((2 * S, R), jnp.float32),
        in_specs=[SMEM, VMEM, VMEM, VMEM, VMEM],
        out_specs=VMEM,
        compiler_params=pltpu.CompilerParams(vmem_limit_bytes=12 << 20),
        cost_estimate=pl.CostEstimate(
            flops=12 * R * S * V, bytes_accessed=8 * S * (R + V), transcendentals=0
        ),
    )(me, high, low, depth, basis)


def leaf_kernel(high, low, depth, basis, out):
    own = masked(basis[0], depth, 0)
    out[...] = dot3(own, split(dot3(own, (high[...], low[...]), 0)), 1)


def leaf(high, low, depth, basis):
    return pl.pallas_call(
        leaf_kernel,
        out_shape=jax.ShapeDtypeStruct((V, R), jnp.float32),
        in_specs=[VMEM] * 4,
        out_specs=VMEM,
        compiler_params=pltpu.CompilerParams(vmem_limit_bytes=12 << 20),
        cost_estimate=pl.CostEstimate(flops=12 * R * S * V, bytes_accessed=4 * V * R, transcendentals=0),
        name="leaf",
    )(high, low, depth, basis)


def image_kernel(work, me, depth, basis, before, *refs):
    pieces, (out, high, low) = refs[:-3], refs[-3:]
    for number, (slot, other, plan) in enumerate(work):
        levels, masks = slots(me[0], (me[0] & 1) ^ other)
        for unit, (piece, start) in enumerate(plan):
            row = pl.multiple_of(UNIT * (unit ^ masks[slot]), UNIT)
            part_high, part_low = split(pieces[piece][start : start + UNIT, :])
            high[number, pl.ds(row, UNIT), :] = part_high
            low[number, pl.ds(row, UNIT), :] = part_low
        own = masked(basis[levels[slot]], depth, levels[slot])
        image = dot3(own, (high[number], low[number]), 1)
        out[...] = (out[...] if number else before[...]) + image


def images(work, me, depth, basis, before, pieces):
    count = len(work)
    return pl.pallas_call(
        functools.partial(image_kernel, work),
        out_shape=jax.ShapeDtypeStruct((V, R), jnp.float32),
        in_specs=[SMEM] + [VMEM] * (3 + len(pieces)),
        out_specs=VMEM,
        scratch_shapes=[pltpu.VMEM((count, S, R), jnp.bfloat16), pltpu.VMEM((count, S, R), jnp.bfloat16)],
        compiler_params=pltpu.CompilerParams(vmem_limit_bytes=12 << 20),
        cost_estimate=pl.CostEstimate(
            flops=count * 6 * R * S * V, bytes_accessed=count * 4 * S * (R + V), transcendentals=0
        ),
    )(me, depth, basis, before, *pieces)


def plan_ab(slot):
    out = []
    for unit in range(UNITS):
        if slot == 0:
            chunk, quarter = unit >> 2, unit & 3
            out.append((chunk, quarter * 48 if chunk < 2 else quarter * UNIT))
        else:
            out.append((unit >> 3, (unit >> 1 & 3) * 48 + UNIT + (unit & 1) * UNIT))
    return out


def shift_pieces(plan, by):
    return [(piece + by, row) for piece, row in plan]


PLAN_C = [(u >> 3, (u & 7) * UNIT) for u in range(UNITS)]
PLAN_D = [(0, u * UNIT) for u in range(UNITS)]


def local(kernel, rows, *arrays):
    return pl.pallas_call(
        kernel,
        out_shape=tuple(jax.ShapeDtypeStruct((height, R), jnp.float32) for height in rows),
        in_specs=[SMEM if array.ndim == 1 else VMEM for array in arrays],
        out_specs=(VMEM,) * len(rows),
        compiler_params=pltpu.CompilerParams(vmem_limit_bytes=4 << 20),
    )(*arrays)


def cut_kernel(kept, got, *outs):
    start = 0
    for out in outs:
        part = slice(start, start + out.shape[0])
        out[...] = kept[part, :] + got[part, :]
        start = part.stop


def join_kernel(base, r1, r2, r3, *outs):
    for quarter, out in enumerate(outs):
        at = quarter * 48
        top = slice(quarter * UNIT, (quarter + 1) * UNIT)
        out[:UNIT, :] = (base[at : at + UNIT, :] + r1[at : at + UNIT, :]) + (r2[top, :] + r3[top, :])
        out[UNIT:, :] = base[at + UNIT : at + 48, :] + r1[at + UNIT : at + 48, :]


def by_core(me, zero, one):
    @pl.when((me[0] & 1) == 0)
    def _():
        zero()

    @pl.when((me[0] & 1) == 1)
    def _():
        one()


def settle_kernel(me, u0, u3, t1, t2, t3, total, passed):
    def zero():
        total[...] = u0[...] + t1[...]
        passed[...] = u3[...] + t2[...]

    def one():
        total[...] = (u0[...] + t1[...]) + (t2[...] + t3[...])
        passed[...] = total[...]

    by_core(me, zero, one)


def finish_kernel(me, total, other, out, passed):
    def zero():
        out[...] = total[...]
        passed[...] = other[...]

    def one():
        out[...] = total[...] + other[...]
        passed[...] = out[...]

    by_core(me, zero, one)


def stack_kernel(me, total, g1, g2, g3, other, done, top):
    for quarter, part in enumerate((total, g1, g2)):
        done[quarter * 48 : (quarter + 1) * 48, :] = part[...]
        top[quarter * UNIT : (quarter + 1) * UNIT, :] = part[:UNIT, :]

    def last(part):
        done[144:, :] = part[...]
        top[48:, :] = part[:UNIT, :]

    by_core(me, lambda: last(other), lambda: last(g3))


def half_kernel(me, c, m2, out):
    def zero():
        out[...] = c[...]

    def one():
        out[...] = c[...] + m2[...]

    by_core(me, zero, one)


def whole_kernel(me, c_low, c_high, m2, m4, out):
    out[:64, :] = c_low[...]

    def zero():
        out[64:, :] = c_high[...] + m2[...]

    def one():
        out[64:, :] = m4[...]

    by_core(me, zero, one)


def steps(basis, rhs, vertex_tier_depth):
    index_here = lax.axis_index("leaf")
    me = index_here.reshape(1)

    send_ab, high, low, depth = first_partials(me, vertex_tier_depth.reshape(1, V), rhs, basis)
    got_ab = send(send_ab, SWAP)
    keep_ab = partials([(0, 0), (1, 0)], me, high, low, depth, basis)

    step = [None] + [pairs(along_y(j), along_x(j)) for j in (1, 2, 3)]
    base, s1, s2, s3 = local(cut_kernel, (192, 192, 64, 64), keep_ab, got_ab)
    r1 = send(s1, step[1])
    r2 = send(s2, step[2])
    r3 = send(s3, step[3])

    send_cd = partials([(2, 1), (3, 1)], me, high, low, depth, basis)
    got_cd = send(send_cd, SWAP)
    keep_cd = partials([(2, 0), (3, 0)], me, high, low, depth, basis)
    near, mid = pairs(along_z(1), shifted_z(1)), pairs(along_z(2), shifted_z(2))
    c_low, c_high, d = local(cut_kernel, (128, 128, 256), keep_cd, got_cd)
    c_low, c_high = local(cut_kernel, (64, 64), c_low, send(c_high, near))
    d = d + send(d, pairs(along_z(1), None))

    u0, u1, u2, u3 = local(join_kernel, (48,) * 4, base, r1, r2, r3)
    t1 = send(u1, pairs(shifted_z(1), along_y(1)))
    t2 = send(u2, pairs(shifted_z(1), along_y(2)))
    t3 = send(u3, pairs(None, along_y(3)))
    total, passed = local(settle_kernel, (48, 48), me, u0, u3, t1, t2, t3)
    total = total + send(passed, pairs(shifted_z(2), along_z(1)))
    total = total + send(total, pairs(along_z(4), along_z(2)))
    other = send(total, pairs(shifted_z(2), along_z(4)))
    total, passed = local(finish_kernel, (48, 48), me, total, other)
    g1 = send(total, pairs(shifted_z(1), along_y(1)))
    g2 = send(passed, pairs(shifted_z(1), along_y(2)))
    g3 = send(total, pairs(None, along_y(3)))
    done, top = local(stack_kernel, (192, 64), me, total, g1, g2, g3, other)
    q1, q2, q3 = send(done, step[1]), send(top, step[2]), send(top, step[3])
    ab_pieces = (done, q1, q2, q3)

    m2 = send(c_high, mid)
    (c_low,) = local(half_kernel, (64,), me, c_low, m2)
    c_low = c_low + send(c_low, pairs(along_z(2), along_z(4)))
    m4 = send(c_low, pairs(None, shifted_z(2)))
    (c_half,) = local(whole_kernel, (128,), me, c_low, c_high, m2, m4)
    c_pieces = (c_half, send(c_half, near))

    their_c = tuple(send(piece, SWAP) for piece in c_pieces)
    their_d = send(d, SWAP)
    their_ab = tuple(send(piece, SWAP) for piece in ab_pieces)

    result = leaf(high, low, depth, basis)
    result = images([(2, 0, PLAN_C), (2, 1, shift_pieces(PLAN_C, 2))], me, depth, basis, result, c_pieces + their_c)
    result = images(
        [(3, 0, PLAN_D), (3, 1, shift_pieces(PLAN_D, 1)), (0, 0, shift_pieces(plan_ab(0), 2)), (1, 0, shift_pieces(plan_ab(1), 2))],
        me, depth, basis, result, (d, their_d) + ab_pieces,
    )
    return images([(0, 1, plan_ab(0)), (1, 1, plan_ab(1))], me, depth, basis, result, their_ab)


def solution(mesh):
    in_specs = (P(None, "leaf", None), P("leaf", None), P("leaf"))
    out_specs = P("leaf", None)
    return jax.shard_map(steps, mesh=mesh, in_specs=in_specs, out_specs=out_specs, check_vma=False)
```

```python
import functools

import jax
import jax.numpy as jnp
from jax import lax
from jax.experimental import pallas as pl
from jax.experimental.pallas import tpu as pltpu
from jax.sharding import PartitionSpec as P


N = 256
V = 512
S = 256
R = 768
UNIT = 16
UNITS = 16
VMEM = pl.BlockSpec(memory_space=pltpu.VMEM)
SMEM = pl.BlockSpec(memory_space=pltpu.SMEM)
HBM = pl.BlockSpec(memory_space=pltpu.HBM)


def place(i):
    return i >> 6, (i >> 4) & 3, (i >> 1) & 7, i & 1


def index(x, y, z, core):
    return x << 6 | y << 4 | z << 1 | core


def pairs(*partners):
    out = []
    for i in range(N):
        x, y, z, core = place(i)
        if partners[core] is not None:
            out.append((i, index(*partners[core](x, y, z), core)))
    return out


def along_x(j):
    return lambda x, y, z: (x ^ j, y, z)


def along_y(j):
    return lambda x, y, z: (x, y ^ j, z)


def along_z(j):
    return lambda x, y, z: (x, y, z ^ j)


def shifted_z(j):
    return lambda x, y, z: (x, y, ((((z + 7) & 7) ^ j) + 1) & 7)


def send(array, perm):
    return lax.ppermute(array, "leaf", perm)


SWAP = [(i, i ^ 1) for i in range(N)]


def slots(me, core):
    x, y, z, _ = place(me)
    turned = (z + 7) & 7
    low, mid = turned & 1, turned >> 1 & 1
    quarter = low ^ 3 * mid
    first = core == 0
    levels = (6 + 2 * core, 5 + 2 * core, 3 + core, 2 - core)
    masks = (
        jnp.where(first, y << 2 | quarter, x << 2 | y),
        jnp.where(first, (y & 1) << 3 | quarter << 1, (x & 1) << 3 | y << 1),
        jnp.where(first, (z & 1) << 3, (low << 1 | mid) << 2),
        jnp.zeros_like(z),
    )
    return levels, masks


def row_a(unit):
    chunk, quarter = unit >> 2, unit & 3
    return jnp.where(chunk < 2, chunk * 192 + quarter * 48, 256 + chunk * 64 + quarter * UNIT)


def row_b(unit):
    return (unit >> 3) * 192 + (unit >> 1 & 3) * 48 + UNIT + (unit & 1) * UNIT


def row_c(unit):
    return unit * UNIT


def row_d(unit):
    return S + unit * UNIT


ROWS = (row_a, row_b, row_c, row_d)


def split(value):
    high = value.astype(jnp.bfloat16)
    low = (value - high.astype(jnp.float32)).astype(jnp.bfloat16)
    return high, low


def masked(basis, depth, level):
    keep = depth[...] >= jnp.asarray(level).astype(jnp.float32)
    return split(
        jnp.concatenate([jnp.where(keep, basis[:, :128], 0.0), jnp.where(keep, basis[:, 128:], 0.0)], 1)
    )


def dot3(a, b, contract):
    dot = functools.partial(
        lax.dot_general,
        dimension_numbers=(((contract,), (0,)), ((), ())),
        preferred_element_type=jnp.float32,
    )
    return dot(a[0], b[0]) + (dot(a[0], b[1]) + dot(a[1], b[0]))


def put(product, out, slot, mask):
    for unit in range(UNITS):
        row = pl.multiple_of(ROWS[slot](unit ^ mask), UNIT)
        out[pl.ds(row, UNIT), :] = product[unit * UNIT : (unit + 1) * UNIT]


def first_kernel(me, depth_hbm, rhs_hbm, basis_hbm, out, high, low, depth_out, depth, rhs, basis, sems):
    levels, masks = slots(me[0], 1 - (me[0] & 1))
    copies = [pltpu.make_async_copy(rhs_hbm, rhs, sems.at[0])]
    for number, slot in enumerate((2, 3)):
        copies.append(pltpu.make_async_copy(basis_hbm.at[levels[slot]], basis.at[number], sems.at[number + 1]))
    depth_copy = pltpu.make_async_copy(depth_hbm, depth, sems.at[3])
    depth_copy.start()
    for copy in copies:
        copy.start()
    depth_copy.wait()
    depth_out[...] = jnp.broadcast_to(depth[...].astype(jnp.float32), (128, V)).T
    copies[0].wait()
    high[...], low[...] = split(rhs[...])
    for number, slot in enumerate((2, 3)):
        copies[number + 1].wait()
        product = dot3(masked(basis.at[number][...], depth_out, levels[slot]), (high[...], low[...]), 0)
        put(product, out, slot, masks[slot])


def first_partials(me, depth, rhs, basis):
    return pl.pallas_call(
        first_kernel,
        out_shape=(
            jax.ShapeDtypeStruct((2 * S, R), jnp.float32),
            jax.ShapeDtypeStruct((V, R), jnp.bfloat16),
            jax.ShapeDtypeStruct((V, R), jnp.bfloat16),
            jax.ShapeDtypeStruct((V, 128), jnp.float32),
        ),
        in_specs=[SMEM, HBM, HBM, HBM],
        out_specs=(VMEM,) * 4,
        scratch_shapes=[
            pltpu.VMEM((1, V), jnp.int32),
            pltpu.VMEM((V, R), jnp.float32),
            pltpu.VMEM((2, V, S), jnp.float32),
            pltpu.SemaphoreType.DMA((4,)),
        ],
        compiler_params=pltpu.CompilerParams(vmem_limit_bytes=50 << 20),
        cost_estimate=pl.CostEstimate(flops=12 * R * S * V, bytes_accessed=2 * 4 * S * (R + V), transcendentals=0),
        name="send_cd",
    )(me, depth, rhs, basis)


def partial_kernel(work, me, high, low, depth, basis, out):
    for slot, other in work:
        levels, masks = slots(me[0], (me[0] & 1) ^ other)
        product = dot3(masked(basis[levels[slot]], depth, levels[slot]), (high[...], low[...]), 0)
        put(product, out, slot, masks[slot])


def partials(work, me, high, low, depth, basis):
    return pl.pallas_call(
        functools.partial(partial_kernel, work),
        out_shape=jax.ShapeDtypeStruct((2 * S, R), jnp.float32),
        in_specs=[SMEM, VMEM, VMEM, VMEM, VMEM],
        out_specs=VMEM,
        compiler_params=pltpu.CompilerParams(vmem_limit_bytes=12 << 20),
        cost_estimate=pl.CostEstimate(
            flops=12 * R * S * V, bytes_accessed=8 * S * (R + V), transcendentals=0
        ),
    )(me, high, low, depth, basis)


def leaf_kernel(high, low, depth, basis, out):
    own = masked(basis[0], depth, 0)
    out[...] = dot3(own, split(dot3(own, (high[...], low[...]), 0)), 1)


def leaf(high, low, depth, basis):
    return pl.pallas_call(
        leaf_kernel,
        out_shape=jax.ShapeDtypeStruct((V, R), jnp.float32),
        in_specs=[VMEM] * 4,
        out_specs=VMEM,
        compiler_params=pltpu.CompilerParams(vmem_limit_bytes=12 << 20),
        cost_estimate=pl.CostEstimate(flops=12 * R * S * V, bytes_accessed=4 * V * R, transcendentals=0),
        name="leaf",
    )(high, low, depth, basis)


def image_kernel(work, me, depth, basis, before, *refs):
    pieces, (out, high, low) = refs[:-3], refs[-3:]
    for number, (slot, other, plan) in enumerate(work):
        levels, masks = slots(me[0], (me[0] & 1) ^ other)
        for unit, (piece, start) in enumerate(plan):
            row = pl.multiple_of(UNIT * (unit ^ masks[slot]), UNIT)
            part_high, part_low = split(pieces[piece][start : start + UNIT, :])
            high[number, pl.ds(row, UNIT), :] = part_high
            low[number, pl.ds(row, UNIT), :] = part_low
        own = masked(basis[levels[slot]], depth, levels[slot])
        image = dot3(own, (high[number], low[number]), 1)
        out[...] = (out[...] if number else before[...]) + image


def images(work, me, depth, basis, before, pieces):
    count = len(work)
    return pl.pallas_call(
        functools.partial(image_kernel, work),
        out_shape=jax.ShapeDtypeStruct((V, R), jnp.float32),
        in_specs=[SMEM] + [VMEM] * (3 + len(pieces)),
        out_specs=VMEM,
        scratch_shapes=[pltpu.VMEM((count, S, R), jnp.bfloat16), pltpu.VMEM((count, S, R), jnp.bfloat16)],
        compiler_params=pltpu.CompilerParams(vmem_limit_bytes=12 << 20),
        cost_estimate=pl.CostEstimate(
            flops=count * 6 * R * S * V, bytes_accessed=count * 4 * S * (R + V), transcendentals=0
        ),
    )(me, depth, basis, before, *pieces)


def plan_ab(slot):
    out = []
    for unit in range(UNITS):
        if slot == 0:
            chunk, quarter = unit >> 2, unit & 3
            out.append((chunk, quarter * 48 if chunk < 2 else quarter * UNIT))
        else:
            out.append((unit >> 3, (unit >> 1 & 3) * 48 + UNIT + (unit & 1) * UNIT))
    return out


def shift_pieces(plan, by):
    return [(piece + by, row) for piece, row in plan]


PLAN_C = [(u >> 3, (u & 7) * UNIT) for u in range(UNITS)]
PLAN_D = [(0, u * UNIT) for u in range(UNITS)]


def local(kernel, rows, *arrays):
    return pl.pallas_call(
        kernel,
        out_shape=tuple(jax.ShapeDtypeStruct((height, R), jnp.float32) for height in rows),
        in_specs=[SMEM if array.ndim == 1 else VMEM for array in arrays],
        out_specs=(VMEM,) * len(rows),
        compiler_params=pltpu.CompilerParams(vmem_limit_bytes=4 << 20),
    )(*arrays)


def cut_kernel(kept, got, *outs):
    start = 0
    for out in outs:
        part = slice(start, start + out.shape[0])
        out[...] = kept[part, :] + got[part, :]
        start = part.stop


def join_kernel(base, r1, r2, r3, *outs):
    for quarter, out in enumerate(outs):
        at = quarter * 48
        top = slice(quarter * UNIT, (quarter + 1) * UNIT)
        out[:UNIT, :] = (base[at : at + UNIT, :] + r1[at : at + UNIT, :]) + (r2[top, :] + r3[top, :])
        out[UNIT:, :] = base[at + UNIT : at + 48, :] + r1[at + UNIT : at + 48, :]


def by_core(me, zero, one):
    @pl.when((me[0] & 1) == 0)
    def _():
        zero()

    @pl.when((me[0] & 1) == 1)
    def _():
        one()


def settle_kernel(me, u0, u3, t1, t2, t3, total, passed):
    def zero():
        total[...] = u0[...] + t1[...]
        passed[...] = u3[...] + t2[...]

    def one():
        total[...] = (u0[...] + t1[...]) + (t2[...] + t3[...])
        passed[...] = total[...]

    by_core(me, zero, one)


def finish_kernel(me, total, far, side, back, out, passed):
    def zero():
        out[...] = total[...] + far[...]
        passed[...] = side[...] + back[...]

    def one():
        out[...] = (total[...] + far[...]) + (side[...] + back[...])
        passed[...] = out[...]

    by_core(me, zero, one)


def stack_kernel(me, total, g1, g2, g3, other, done, top):
    for quarter, part in enumerate((total, g1, g2)):
        done[quarter * 48 : (quarter + 1) * 48, :] = part[...]
        top[quarter * UNIT : (quarter + 1) * UNIT, :] = part[:UNIT, :]

    def last(part):
        done[144:, :] = part[...]
        top[48:, :] = part[:UNIT, :]

    by_core(me, lambda: last(other), lambda: last(g3))


def half_kernel(me, c, m2, out):
    def zero():
        out[...] = c[...]

    def one():
        out[...] = c[...] + m2[...]

    by_core(me, zero, one)


def whole_kernel(me, c_low, c_high, m2, m4, out):
    def zero():
        out[:64, :] = c_low[...] + m4[...]
        out[64:, :] = c_high[...] + m2[...]

    def one():
        out[:64, :] = c_low[...]
        out[64:, :] = m4[...]

    by_core(me, zero, one)


def steps(basis, rhs, vertex_tier_depth):
    index_here = lax.axis_index("leaf")
    me = index_here.reshape(1)

    send_cd, high, low, depth = first_partials(me, vertex_tier_depth.reshape(1, V), rhs, basis)
    got_cd = send(send_cd, SWAP)
    send_ab = partials([(0, 1), (1, 1)], me, high, low, depth, basis)
    got_ab = send(send_ab, SWAP)
    keep_cd = partials([(2, 0), (3, 0)], me, high, low, depth, basis)

    near, mid = pairs(along_z(1), shifted_z(1)), pairs(along_z(2), shifted_z(2))
    c_low, c_high, d = local(cut_kernel, (128, 128, 256), keep_cd, got_cd)

    keep_ab = partials([(0, 0), (1, 0)], me, high, low, depth, basis)
    step = [None] + [pairs(along_y(j), along_x(j)) for j in (1, 2, 3)]
    base, s1, s2, s3 = local(cut_kernel, (192, 192, 64, 64), keep_ab, got_ab)
    r1 = send(s1, step[1])
    r2 = send(s2, step[2])
    r3 = send(s3, step[3])
    c_low, c_high = local(cut_kernel, (64, 64), c_low, send(c_high, near))
    d = d + send(d, pairs(along_z(1), None))

    u0, u1, u2, u3 = local(join_kernel, (48,) * 4, base, r1, r2, r3)
    t1 = send(u1, pairs(shifted_z(1), along_y(1)))
    t2 = send(u2, pairs(shifted_z(1), along_y(2)))
    t3 = send(u3, pairs(None, along_y(3)))
    total, passed = local(settle_kernel, (48, 48), me, u0, u3, t1, t2, t3)
    total = total + send(passed, pairs(shifted_z(2), along_z(1)))
    far = send(total, pairs(along_z(4), along_z(4)))
    side = send(total, pairs(shifted_z(2), along_z(2)))
    back = send(total, pairs(shifted_z(6), along_z(6)))
    total, passed = local(finish_kernel, (48, 48), me, total, far, side, back)
    g1 = send(total, pairs(shifted_z(1), along_y(1)))
    g2 = send(passed, pairs(shifted_z(1), along_y(2)))
    g3 = send(total, pairs(None, along_y(3)))
    done, top = local(stack_kernel, (192, 64), me, total, g1, g2, g3, passed)
    q1, q2, q3 = send(done, step[1]), send(top, step[2]), send(top, step[3])
    ab_pieces = (done, q1, q2, q3)

    m2 = send(c_high, mid)
    (c_low,) = local(half_kernel, (64,), me, c_low, m2)
    c_low = c_low + send(c_low, pairs(None, along_z(4)))
    m4 = send(c_low, mid)
    (c_half,) = local(whole_kernel, (128,), me, c_low, c_high, m2, m4)
    c_pieces = (c_half, send(c_half, near))

    their_c = tuple(send(piece, SWAP) for piece in c_pieces)
    their_d = send(d, SWAP)
    their_ab = tuple(send(piece, SWAP) for piece in ab_pieces)

    result = leaf(high, low, depth, basis)
    own_ab, their_plan = [(0, 0, plan_ab(0)), (1, 0, plan_ab(1))], [(0, 1, plan_ab(0)), (1, 1, plan_ab(1))]
    result = images([(3, 0, PLAN_D), (3, 1, shift_pieces(PLAN_D, 1))], me, depth, basis, result, (d, their_d))
    own_ab, their_plan = [(0, 0, plan_ab(0)), (1, 0, plan_ab(1))], [(0, 1, plan_ab(0)), (1, 1, plan_ab(1))]
    result = images(own_ab + [(2, 0, shift_pieces(PLAN_C, 4))], me, depth, basis, result, ab_pieces + c_pieces)
    return images(their_plan + [(2, 1, shift_pieces(PLAN_C, 4))], me, depth, basis, result, their_ab + their_c)


def solution(mesh):
    in_specs = (P(None, "leaf", None), P("leaf", None), P("leaf"))
    out_specs = P("leaf", None)
    return jax.shard_map(steps, mesh=mesh, in_specs=in_specs, out_specs=out_specs, check_vma=False)
```
